32 devices in a mesh: row: 8 (over y, x, core), col: 4 (over z).
Axes of the slice: x: 2, y: 2, z: 4, core: 2. Of those that a mesh axis runs over, the one named last changes fastest.
Arguments:
- coeffs: float32 [2, 12288, 2048], P(None, ('row', 'col')), may hold values from -6 to 6
- forces: float32 [2, 12288, 2048], P(None, ('row', 'col')), may hold values from -6 to 6
- multipliers: float32 [2048, 2048], P('row', 'col'), may hold values from -0.125 to 0.125
Outputs:
- constrained: float32 [2, 12288, 2048], P(None, ('row', 'col'))
The draws below stay inside these ranges and needn't reach their ends.
All inputs are finite; a program needn't handle non-finite values.
Results may differ from the reference program's by a relative error of at most 0.000051.
Values sent between devices are 32-bit elements; how exact they have to be, the bound alone decides.
A program may use at most 128 MiB of HBM per device.

```python
import jax
import jax.numpy as jnp
from jax import lax

ORB = 2048
COEFS = 12288


def level_of(stream_key, extent, cuts, least, largest):
    gain = 1.0
    for position, shards_of in cuts:
        draws = jax.random.uniform(jax.random.fold_in(jax.random.fold_in(stream_key, 6), position), (shards_of,), jnp.float32, least / len(cuts), largest / len(cuts))
        gain = gain * jnp.repeat(jnp.exp(draws), extent[position] // shards_of).reshape((-1,) + (1,) * (len(extent) - 1 - position))
    return gain


def scatter_about(rng, extent, deviation, reach, shards=(), kind=jnp.bfloat16):
    level = level_of(rng, extent, shards, -0.22, 0.18) if shards else 1.0
    array = jax.random.normal(rng, extent, jnp.float32) * deviation * level
    return jnp.minimum(jnp.maximum(array, -reach), reach).astype(kind)


def setup_inputs(seed: int = 0) -> dict:
    keys = jax.random.split(jax.random.key(seed), 4)
    return {
        "coeffs": scatter_about(keys[0], (2, COEFS, ORB), 1.0, 6.0, ((1, 32),), jnp.float32),
        "forces": scatter_about(keys[1], (2, COEFS, ORB), 1.0, 6.0, ((1, 32),), jnp.float32),
        "multipliers": scatter_about(keys[2], (ORB, ORB), ORB ** -0.5, 0.125, ((0, 8), (1, 4)), jnp.float32),
    }


def reference(coeffs, forces, multipliers):
    stacked = coeffs.reshape(2 * coeffs.shape[1], coeffs.shape[2])
    product = jnp.dot(stacked, multipliers, precision=lax.Precision.HIGHEST, preferred_element_type=jnp.float32)
    return forces - product.reshape(coeffs.shape)
```

```python
import functools

import jax
import jax.numpy as jnp
from jax import lax
from jax.experimental import pallas as pl
from jax.experimental.pallas import tpu as pltpu
from jax.sharding import PartitionSpec as P

MESH = pl.DeviceIdType.MESH
CORES, XS = 2, 2
ORDERS = ("zxy", "zyx", "xzy", "yzx")


def pieces_of(depth):
    small = depth * 3 // 16
    large = depth // 2 - small
    cuts, start = [], 0
    for rows in (small, small, large, large):
        cuts.append((start, rows))
        start += rows
    return cuts


def kernel(rows, cols, coeffs, forces, block, out, lam, staged, high, low, total, lam_high, lam_low,
           local_sem, out_sem, near_send, z_send, pair_send, recv, pair_recv):
    ys = rows // (CORES * XS)
    depth, width = block.shape
    half = coeffs.shape[1]
    pieces = pieces_of(depth)
    row, z = lax.axis_index("row"), lax.axis_index("col")
    core, x, y = lax.rem(row, CORES), lax.rem(row // CORES, XS), row // (CORES * XS)

    def row_at(dy, dx, of_core=core):
        return (lax.rem(y + dy, ys) * XS + lax.rem(x + dx, XS)) * CORES + of_core

    def base(r, c):
        return (c * rows + r) * depth

    own = pltpu.make_async_copy(block, lam.at[pl.ds(pl.multiple_of(base(row, z), 8), depth)], local_sem.at[0])
    own.start()
    loads = []
    for part in range(2):
        load = pltpu.make_async_copy(coeffs.at[part], staged.at[pl.ds(part * half, half)], local_sem.at[1 + part])
        load.start()
        loads.append(load)
    for part in range(2):
        for c in range(cols):
            load = pltpu.make_async_copy(
                forces.at[part, :, pl.ds(c * width, width)],
                total.at[c, pl.ds(part * half, half)],
                local_sem.at[3 + part * cols + c],
            )
            load.start()
            loads.append(load)

    near = [(0, 1)] + [(dy, 0) for dy in range(1, ys)]
    targets = [row_at(dy, dx) for dy, dx in near]
    partner = row + 1 - 2 * core
    barrier = pltpu.get_barrier_semaphore()
    for target in targets + [partner]:
        pl.semaphore_signal(barrier, inc=1, device_id={"row": target, "col": z}, device_id_type=MESH)

    @pl.when(z > 0)
    def _():
        pl.semaphore_signal(barrier, inc=1, device_id={"row": row, "col": z - 1}, device_id_type=MESH)

    @pl.when(z < cols - 1)
    def _():
        pl.semaphore_signal(barrier, inc=1, device_id={"row": row, "col": z + 1}, device_id_type=MESH)

    along = jnp.where(z > 0, 1, 0) + jnp.where(z < cols - 1, 1, 0)
    pl.semaphore_wait(barrier, len(near) + 1 + along)
    own.wait()

    def piece_copy(kind, r, c, send_sem, to_row, to_col):
        start, count = pieces[kind]
        place = lam.at[pl.ds(pl.multiple_of(base(r, c) + start, 8), count)]
        return pltpu.make_async_remote_copy(
            src_ref=place, dst_ref=place, send_sem=send_sem, recv_sem=recv.at[kind, r // CORES, c],
            device_id={"row": to_row, "col": to_col}, device_id_type=MESH,
        )

    sent = [0] * len(near)

    def take(kind, dy, dx, c, first):
        r = row_at(dy, dx)
        if not (first and dy == 0 and dx == 0):
            piece_copy(kind, r, c, near_send.at[0], row, z).wait_recv()
        order = ORDERS[kind]
        came = {"x": dx != 0, "y": dy != 0, "z": not first}
        last = max([order.index(axis) for axis in "xyz" if came[axis]], default=-1)
        if order.index("z") > last:
            @pl.when(z > 0)
            def _():
                piece_copy(kind, r, c, z_send.at[0, c], row, z - 1).start()

            @pl.when(z < cols - 1)
            def _():
                piece_copy(kind, r, c, z_send.at[1, c], row, z + 1).start()
        elif order.index("z") == last:
            @pl.when((c > z) & (z > 0))
            def _():
                piece_copy(kind, r, c, z_send.at[0, c], row, z - 1).start()

            @pl.when((c < z) & (z < cols - 1))
            def _():
                piece_copy(kind, r, c, z_send.at[1, c], row, z + 1).start()
        for way, (sy, sx) in enumerate(near):
            if order.index("x" if sx else "y") > last:
                piece_copy(kind, r, c, near_send.at[way], targets[way], z).start()

    def spread(c, first):
        for kind in range(4):
            take(kind, 0, 0, c, first)
        if first:
            take(2, 0, 1, c, first)
            for dy in range(1, ys):
                take(3, dy, 0, c, first)
        take(0, 0, 1, c, first)
        for dy in range(1, ys):
            take(1, dy, 0, c, first)
        if not first:
            take(2, 0, 1, c, first)
            for dy in range(1, ys):
                take(3, dy, 0, c, first)

    def pair_copy(r, c):
        place = lam.at[pl.ds(pl.multiple_of(base(r, c), 8), depth)]
        return pltpu.make_async_remote_copy(
            src_ref=place, dst_ref=place, send_sem=pair_send, recv_sem=pair_recv.at[r // CORES, c],
            device_id={"row": partner, "col": z}, device_id_type=MESH,
        )

    def multiply(r, c):
        held = lam[pl.ds(pl.multiple_of(base(r, c), 8), depth), :]
        rounded = held.astype(jnp.bfloat16)
        lam_high[...] = rounded
        lam_low[...] = (held - rounded.astype(jnp.float32)).astype(jnp.bfloat16)

        @pl.loop(0, 2)
        def _(part):
            here = pl.ds(pl.multiple_of(part * half, 8), half)
            a_high, a_low = high[r, here, :], low[r, here, :]
            product = jnp.dot(a_high, lam_high[...], preferred_element_type=jnp.float32)
            product += jnp.dot(a_high, lam_low[...], preferred_element_type=jnp.float32)
            product += jnp.dot(a_low, lam_high[...], preferred_element_type=jnp.float32)
            total[c, here, :] -= product

    def store(c):
        return [
            pltpu.make_async_copy(
                total.at[c, pl.ds(part * half, half)],
                out.at[part, :, pl.ds(pl.multiple_of(c * width, 128), width)],
                out_sem.at[part, c],
            )
            for part in range(2)
        ]

    def finish(c, first):
        pair_copy(row, c).start()
        for kind in (1, 3):
            take(kind, 0, 1, c, first)
        pair_copy(row_at(0, 1), c).start()
        for dy in range(1, ys):
            for kind in (0, 2):
                take(kind, dy, 0, c, first)
            pair_copy(row_at(dy, 0), c).start()
        for dy in range(1, ys):
            for kind in range(4):
                take(kind, dy, 1, c, first)
            pair_copy(row_at(dy, 1), c).start()

        @pl.loop(0, rows // CORES)
        def _(q):
            multiply(q * CORES + core, c)

        @pl.loop(0, rows // CORES)
        def _(q):
            r = q * CORES + 1 - core
            pair_copy(r, c).wait_recv()
            multiply(r, c)

        for copy in store(c):
            copy.start()

    def column(j):
        edge = jnp.minimum(z, cols - 1 - z)
        longer = jnp.where(z < cols // 2, 1, -1)
        near_by = longer * (1 - 2 * lax.rem(j + 1, 2)) * ((j + 1) // 2)
        return z + jnp.where(j <= 2 * edge, near_by, longer * (j - edge))

    spread(z, True)
    for load in loads:
        load.wait()
    for r in range(rows):
        value = staged[:, r * depth:(r + 1) * depth]
        rounded = value.astype(jnp.bfloat16)
        high[r] = rounded
        low[r] = (value - rounded.astype(jnp.float32)).astype(jnp.bfloat16)

    spread(column(1), False)
    finish(z, True)

    @pl.loop(2, cols)
    def _(j):
        spread(column(j), False)
        finish(column(j - 1), False)

    finish(column(cols - 1), False)

    def drain(count, sem):
        span = lam.at[pl.ds(0, count)]
        pltpu.make_async_remote_copy(
            src_ref=span, dst_ref=span, send_sem=sem, recv_sem=recv.at[0, 0, 0],
            device_id={"row": partner, "col": z}, device_id_type=MESH,
        ).wait_send()

    small, large = pieces[0][1], pieces[2][1]
    for way, (sy, sx) in enumerate(near):
        if sx:
            count = cols * small + cols * ys * small + large + cols * ys * large
        else:
            count = cols * XS * small + cols * small + cols * XS * large + large
        drain(count, near_send.at[way])
    drain(cols * (rows // CORES) * depth, pair_send)
    along_z = 2 * small + XS * large + ys * large

    @pl.loop(0, cols)
    def _(c):
        @pl.when((c >= z) & (z > 0))
        def _():
            drain(along_z, z_send.at[0, c])

        @pl.when((c <= z) & (z < cols - 1))
        def _():
            drain(along_z, z_send.at[1, c])

        for copy in store(c):
            copy.wait()


def body(rows, cols, coeffs, forces, multipliers):
    parts, half, orbitals = coeffs.shape
    depth, width = multipliers.shape
    count = parts * half
    near = rows // (CORES * XS)
    return pl.pallas_call(
        functools.partial(kernel, rows, cols),
        out_shape=jax.ShapeDtypeStruct(coeffs.shape, jnp.float32),
        in_specs=[pl.BlockSpec(memory_space=pl.ANY)] * 3,
        out_specs=pl.BlockSpec(memory_space=pl.ANY),
        scratch_shapes=[
            pltpu.VMEM((rows * cols * depth, width), jnp.float32),
            pltpu.VMEM((count, orbitals), jnp.float32),
            pltpu.VMEM((rows, count, depth), jnp.bfloat16),
            pltpu.VMEM((rows, count, depth), jnp.bfloat16),
            pltpu.VMEM((cols, count, width), jnp.float32),
            pltpu.VMEM((depth, width), jnp.bfloat16),
            pltpu.VMEM((depth, width), jnp.bfloat16),
            pltpu.SemaphoreType.DMA((3 + 2 * cols,)),
            pltpu.SemaphoreType.DMA((2, cols)),
            pltpu.SemaphoreType.DMA((near,)),
            pltpu.SemaphoreType.DMA((2, cols)),
            pltpu.SemaphoreType.DMA,
            pltpu.SemaphoreType.DMA((4, rows // CORES, cols)),
            pltpu.SemaphoreType.DMA((rows // CORES, cols)),
        ],
        compiler_params=pltpu.CompilerParams(
            collective_id=0, has_side_effects=True, vmem_limit_bytes=60 * 1024 * 1024
        ),
    )(coeffs, forces, multipliers)


def solution(mesh):
    placed = (P(None, ("row", "col"), None), P(None, ("row", "col"), None), P("row", "col"))
    rows, cols = mesh.shape["row"], mesh.shape["col"]
    return jax.shard_map(
        functools.partial(body, rows, cols), mesh=mesh, in_specs=placed,
        out_specs=P(None, ("row", "col"), None), check_vma=False,
    )
```

```python
import functools

import jax
import jax.numpy as jnp
from jax import lax
from jax.experimental import pallas as pl
from jax.experimental.pallas import tpu as pltpu
from jax.sharding import PartitionSpec as P

MESH = pl.DeviceIdType.MESH
CORES, XS = 2, 2
ORDERS = ("zxy", "zyx", "xzy", "yzx")


def pieces_of(depth):
    small = depth * 3 // 16
    large = depth // 2 - small
    cuts, start = [], 0
    for rows in (small, small, large, large):
        cuts.append((start, rows))
        start += rows
    return cuts


def kernel(rows, cols, coeffs, forces, block, out, lam, staged, high, low, lam_high, lam_low,
           local_sem, near_send, z_send, pair_send, recv, pair_recv):
    ys = rows // (CORES * XS)
    depth, width = block.shape
    half = coeffs.shape[1]
    pieces = pieces_of(depth)
    row, z = lax.axis_index("row"), lax.axis_index("col")
    core, x, y = lax.rem(row, CORES), lax.rem(row // CORES, XS), row // (CORES * XS)

    def row_at(dy, dx, of_core=core):
        return (lax.rem(y + dy, ys) * XS + lax.rem(x + dx, XS)) * CORES + of_core

    def base(r, c):
        return (c * rows + r) * depth

    own = pltpu.make_async_copy(block, lam.at[pl.ds(pl.multiple_of(base(row, z), 8), depth)], local_sem.at[0])
    own.start()
    loads = []
    for part in range(2):
        load = pltpu.make_async_copy(coeffs.at[part], staged.at[pl.ds(part * half, half)], local_sem.at[1 + part])
        load.start()
        loads.append(load)
    for part in range(2):
        load = pltpu.make_async_copy(forces.at[part], out.at[part], local_sem.at[3 + part])
        load.start()
        loads.append(load)

    near = [(0, 1)] + [(dy, 0) for dy in range(1, ys)]
    targets = [row_at(dy, dx) for dy, dx in near]
    partner = row + 1 - 2 * core
    barrier = pltpu.get_barrier_semaphore()
    for target in targets + [partner]:
        pl.semaphore_signal(barrier, inc=1, device_id={"row": target, "col": z}, device_id_type=MESH)

    @pl.when(z > 0)
    def _():
        pl.semaphore_signal(barrier, inc=1, device_id={"row": row, "col": z - 1}, device_id_type=MESH)

    @pl.when(z < cols - 1)
    def _():
        pl.semaphore_signal(barrier, inc=1, device_id={"row": row, "col": z + 1}, device_id_type=MESH)

    along = jnp.where(z > 0, 1, 0) + jnp.where(z < cols - 1, 1, 0)
    pl.semaphore_wait(barrier, len(near) + 1 + along)
    own.wait()

    def piece_copy(kind, r, c, send_sem, to_row, to_col):
        start, count = pieces[kind]
        place = lam.at[pl.ds(pl.multiple_of(base(r, c) + start, 8), count)]
        return pltpu.make_async_remote_copy(
            src_ref=place, dst_ref=place, send_sem=send_sem, recv_sem=recv.at[kind, r // CORES, c],
            device_id={"row": to_row, "col": to_col}, device_id_type=MESH,
        )

    sent = [0] * len(near)

    def take(kind, dy, dx, c, first):
        r = row_at(dy, dx)
        if not (first and dy == 0 and dx == 0):
            piece_copy(kind, r, c, near_send.at[0], row, z).wait_recv()
        order = ORDERS[kind]
        came = {"x": dx != 0, "y": dy != 0, "z": not first}
        last = max([order.index(axis) for axis in "xyz" if came[axis]], default=-1)
        if order.index("z") > last:
            @pl.when(z > 0)
            def _():
                piece_copy(kind, r, c, z_send.at[0, c], row, z - 1).start()

            @pl.when(z < cols - 1)
            def _():
                piece_copy(kind, r, c, z_send.at[1, c], row, z + 1).start()
        elif order.index("z") == last:
            @pl.when((c > z) & (z > 0))
            def _():
                piece_copy(kind, r, c, z_send.at[0, c], row, z - 1).start()

            @pl.when((c < z) & (z < cols - 1))
            def _():
                piece_copy(kind, r, c, z_send.at[1, c], row, z + 1).start()
        for way, (sy, sx) in enumerate(near):
            if order.index("x" if sx else "y") > last:
                piece_copy(kind, r, c, near_send.at[way], targets[way], z).start()

    def spread(c, first, fill):
        for kind in (0, 1):
            take(kind, 0, 0, c, first)
        fill(0)
        for kind in (2, 3):
            take(kind, 0, 0, c, first)
            fill(kind - 1)
        if first:
            take(2, 0, 1, c, first)
            for dy in range(1, ys):
                take(3, dy, 0, c, first)
        take(0, 0, 1, c, first)
        for dy in range(1, ys):
            take(1, dy, 0, c, first)
        fill(3)
        if not first:
            take(2, 0, 1, c, first)
            fill(4)
            for dy in range(1, ys):
                take(3, dy, 0, c, first)

    def pair_copy(r, c):
        place = lam.at[pl.ds(pl.multiple_of(base(r, c), 8), depth)]
        return pltpu.make_async_remote_copy(
            src_ref=place, dst_ref=place, send_sem=pair_send, recv_sem=pair_recv.at[r // CORES, c],
            device_id={"row": partner, "col": z}, device_id_type=MESH,
        )

    def multiply(r, c):
        held = lam[pl.ds(pl.multiple_of(base(r, c), 8), depth), :]
        rounded = held.astype(jnp.bfloat16)
        lam_high[...] = rounded
        lam_low[...] = (held - rounded.astype(jnp.float32)).astype(jnp.bfloat16)

        @pl.loop(0, 2)
        def _(part):
            here = pl.ds(pl.multiple_of(part * half, 8), half)
            a_high, a_low = high[r, here, :], low[r, here, :]
            product = jnp.dot(a_high, lam_high[...], preferred_element_type=jnp.float32)
            product += jnp.dot(a_high, lam_low[...], preferred_element_type=jnp.float32)
            product += jnp.dot(a_low, lam_high[...], preferred_element_type=jnp.float32)
            out[part, :, pl.ds(pl.multiple_of(c * width, 128), width)] -= product

    def settle(c, first, own, other):
        pair_copy(row, c).start()
        own(0, 0)
        for kind in (1, 3):
            take(kind, 0, 1, c, first)
        pair_copy(row_at(0, 1), c).start()
        own(0, 1)
        other(0, 0)
        for dy in range(1, ys):
            for kind in (0, 2):
                take(kind, dy, 0, c, first)
            pair_copy(row_at(dy, 0), c).start()
            own(dy, 0)
        other(0, 1)
        for dy in range(1, ys):
            for kind in range(4):
                take(kind, dy, 1, c, first)
            pair_copy(row_at(dy, 1), c).start()
            own(dy, 1)
        for dy in range(1, ys):
            other(dy, 0)
            other(dy, 1)

    def own_block(c):
        return lambda dy, dx: multiply(row_at(dy, dx), c)

    def other_block(c):
        def run(dy, dx):
            r = row_at(dy, dx, 1 - core)
            pair_copy(r, c).wait_recv()
            multiply(r, c)
        return run

    def fill_with(c, first):
        places = [(dy, dx) for dy in range(ys) for dx in range(XS)]
        work = [(own_block(c), place) for place in places] + [(other_block(c), place) for place in places]

        def fill(turn):
            if turn == 0:
                settle(c, first, lambda *_: None, lambda *_: None)
            else:
                share = len(work) // 4
                for run, place in work[(turn - 1) * share:turn * share]:
                    run(*place)
        return fill

    def column(j):
        edge = jnp.minimum(z, cols - 1 - z)
        longer = jnp.where(z < cols // 2, 1, -1)
        near_by = longer * (1 - 2 * lax.rem(j + 1, 2)) * ((j + 1) // 2)
        return z + jnp.where(j <= 2 * edge, near_by, longer * (j - edge))

    spread(z, True, lambda turn: None)
    for load in loads:
        load.wait()
    for r in range(rows):
        value = staged[:, r * depth:(r + 1) * depth]
        rounded = value.astype(jnp.bfloat16)
        high[r] = rounded
        low[r] = (value - rounded.astype(jnp.float32)).astype(jnp.bfloat16)

    def step(j, first):
        c = column(j - 1)
        spread(column(j), False, fill_with(c, first))

    step(1, True)

    @pl.loop(2, cols)
    def _(j):
        step(j, False)

    last = column(cols - 1)
    settle(last, False, own_block(last), other_block(last))

    def drain(count, sem):
        span = lam.at[pl.ds(0, count)]
        pltpu.make_async_remote_copy(
            src_ref=span, dst_ref=span, send_sem=sem, recv_sem=recv.at[0, 0, 0],
            device_id={"row": partner, "col": z}, device_id_type=MESH,
        ).wait_send()

    small, large = pieces[0][1], pieces[2][1]
    for way, (sy, sx) in enumerate(near):
        if sx:
            count = cols * small + cols * ys * small + large + cols * ys * large
        else:
            count = cols * XS * small + cols * small + cols * XS * large + large
        drain(count, near_send.at[way])
    drain(cols * (rows // CORES) * depth, pair_send)
    along_z = 2 * small + XS * large + ys * large

    @pl.loop(0, cols)
    def _(c):
        @pl.when((c >= z) & (z > 0))
        def _():
            drain(along_z, z_send.at[0, c])

        @pl.when((c <= z) & (z < cols - 1))
        def _():
            drain(along_z, z_send.at[1, c])


def body(rows, cols, coeffs, forces, multipliers):
    parts, half, orbitals = coeffs.shape
    depth, width = multipliers.shape
    count = parts * half
    near = rows // (CORES * XS)
    return pl.pallas_call(
        functools.partial(kernel, rows, cols),
        out_shape=pltpu.VMEM(coeffs.shape, jnp.float32),
        in_specs=[pl.BlockSpec(memory_space=pltpu.HBM)] * 3,
        out_specs=pl.BlockSpec(memory_space=pltpu.VMEM),
        scratch_shapes=[
            pltpu.VMEM((rows * cols * depth, width), jnp.float32),
            pltpu.VMEM((count, orbitals), jnp.float32),
            pltpu.VMEM((rows, count, depth), jnp.bfloat16),
            pltpu.VMEM((rows, count, depth), jnp.bfloat16),
            pltpu.VMEM((depth, width), jnp.bfloat16),
            pltpu.VMEM((depth, width), jnp.bfloat16),
            pltpu.SemaphoreType.DMA((5,)),
            pltpu.SemaphoreType.DMA((near,)),
            pltpu.SemaphoreType.DMA((2, cols)),
            pltpu.SemaphoreType.DMA,
            pltpu.SemaphoreType.DMA((4, rows // CORES, cols)),
            pltpu.SemaphoreType.DMA((rows // CORES, cols)),
        ],
        compiler_params=pltpu.CompilerParams(
            collective_id=0, has_side_effects=True, vmem_limit_bytes=48 * 1024 * 1024
        ),
    )(coeffs, forces, multipliers)


def solution(mesh):
    placed = (P(None, ("row", "col"), None), P(None, ("row", "col"), None), P("row", "col"))
    rows, cols = mesh.shape["row"], mesh.shape["col"]
    return jax.shard_map(
        functools.partial(body, rows, cols), mesh=mesh, in_specs=placed,
        out_specs=P(None, ("row", "col"), None), check_vma=False,
    )
```
